32 devices in a mesh: gx: 4 (over y, core), gy: 8 (over z, x).
Axes of the slice: x: 2, y: 2, z: 4, core: 2. Of those that a mesh axis runs over, the one named last changes fastest.
Arguments:
- spectra: bfloat16 [4, 8, 3, 2, 128, 4096], P('gx', 'gy'), may hold values from -1000 to 1000
- partner_codes: int32 [4, 8, 5], P('gx', 'gy'), may hold values from -1 to 4, as said below
- range_bits: int32 [4, 8, 5, 128, 5], P('gx', 'gy'), may hold values from 0 to 1073741823
- old_stacks: float32 [4, 8, 5, 8, 2, 128, 128], P('gx', 'gy'), may hold values from -6 to 6
Outputs:
- stacks: float32 [4, 8, 5, 8, 2, 128, 128], P('gx', 'gy')
The draws below stay inside these ranges and needn't reach their ends.
Inputs may be any that keep to these rules, and one draw needn't show every extreme that they name: `partner_codes`: each block lists code 0 first, then further distinct codes in increasing order, then -1 in the remaining slots; no listed code names a block outside the grid of 4 x 8 blocks; some block lists all 5 codes.
All inputs are finite; a program needn't handle non-finite values.
Results may differ from the reference program's by a relative error of at most 0.0014.
Values may be sent and summed in bfloat16 or wider, within the bound.
No kernel may reach another device: no remote copies, remote signals or barrier semaphores. Data moves between devices by JAX's collectives and lax.ppermute only.
A program may use at most 192 MiB of HBM per device.

```python
import math
import jax
import jax.numpy as jnp
from jax import lax

ST = 128
F = 4096
BANDS = 8
SLOTS = 5
SEG = 3
BW = 512
WORDS = 5
NBX = 4
NBY = 8


def draw_spectra(key, part):
    first_key = jax.random.fold_in(key, 11)
    second_key = jax.random.fold_in(key, 12)
    third_key = jax.random.fold_in(key, 13)
    full_shape = (NBX, NBY, SEG, 2, ST, F)
    base_noise = jax.random.truncated_normal(first_key, -6.0, 6.0, full_shape, jnp.float32)
    spread = math.log(10.0)
    bin_scale = jnp.exp(spread * jax.random.uniform(second_key, (NBX, NBY, SEG, 1, ST, F), jnp.float32))
    band_scale = jnp.exp(math.log(10.0) * jax.random.uniform(third_key, (NBX, NBY, 1, 1, ST, BANDS, 1), jnp.float32))
    band_full = jnp.broadcast_to(band_scale, (NBX, NBY, 1, 1, ST, BANDS, BW)).reshape(NBX, NBY, 1, 1, ST, F)
    return (base_noise * bin_scale * band_full).astype(jnp.bfloat16)


def draw_partner_codes(key, part):
    row_pos = jnp.arange(NBX, dtype=jnp.int32)[:, None]
    col_pos = jnp.arange(NBY, dtype=jnp.int32)[None, :]
    first_level = jax.random.randint(jax.random.fold_in(key, 21), (NBX, NBY), 0, 10, dtype=jnp.int32)
    second_level = jax.random.randint(jax.random.fold_in(key, 22), (NBX, NBY), 0, 10, dtype=jnp.int32)
    density = first_level * second_level + first_level + second_level + 1
    trials = jax.random.randint(jax.random.fold_in(key, 23), (NBX, NBY, 4), 0, 100, dtype=jnp.int32)
    forced_row = jax.random.randint(jax.random.fold_in(key, 24), (), 1, NBX - 1, dtype=jnp.int32)
    forced_col = jax.random.randint(jax.random.fold_in(key, 25), (), 0, NBY - 1, dtype=jnp.int32)
    forced = (row_pos == forced_row) & (col_pos == forced_col)
    step_rows = [1, -1, 0, 1]
    step_cols = [0, 1, 1, 1]
    listed = [jnp.ones((NBX, NBY), dtype=bool)]
    for which in range(4):
        target_row = row_pos + step_rows[which]
        target_col = col_pos + step_cols[which]
        inside = (target_row >= 0) & (target_row < NBX) & (target_col < NBY)
        listed.append(inside & ((trials[:, :, which] < density) | forced))
    valid = jnp.stack(listed, -1).astype(jnp.int32)
    ranks = jnp.cumsum(valid, -1) - 1
    counts = jnp.sum(valid, -1)
    code_values = jnp.arange(5, dtype=jnp.int32)
    slots_out = []
    for slot_index in range(SLOTS):
        matched = valid * (ranks == slot_index).astype(jnp.int32)
        chosen = jnp.sum(matched * code_values, -1)
        slots_out.append(jnp.where(counts > slot_index, chosen, -1).astype(jnp.int32))
    return jnp.stack(slots_out, -1)


def touch_ends(drawn, key, smallest, largest):
    spot = [jax.random.randint(jax.random.fold_in(key, axis), (), 0, length) for axis, length in enumerate(drawn.shape)]
    widest = drawn.shape.index(max(drawn.shape))
    neighbour = spot[:widest] + [(spot[widest] + 1) % drawn.shape[widest]] + spot[widest + 1:]
    return drawn.at[tuple(spot)].set(smallest).at[tuple(neighbour)].set(largest)


def shard_levels(rng, extent, pieces, smallest, top_value):
    loudness, own = 1.0, jax.random.fold_in(rng, 6)
    for axis_at, shards_of in pieces:
        heights = jnp.exp(jax.random.uniform(jax.random.fold_in(own, axis_at), (shards_of,), jnp.float32, smallest / len(pieces), top_value / len(pieces)))
        loudness = loudness * jnp.repeat(heights, extent[axis_at] // shards_of).reshape([-1 if axis == axis_at else 1 for axis in range(len(extent))])
    return loudness


def centred(own_key, dims, width, limit, cuts=(), kind=jnp.bfloat16):
    array = width * jax.random.normal(own_key, dims, jnp.float32)
    if cuts:
        array = array * shard_levels(own_key, dims, cuts, -0.22, 0.18)
    return jnp.clip(array, -limit, limit).astype(kind)


def setup_inputs(seed: int = 0) -> dict:
    keys = jax.random.split(jax.random.key(seed), 5)
    return {
        "spectra": draw_spectra(jax.random.fold_in(keys[4], 71), 0),
        "partner_codes": draw_partner_codes(jax.random.fold_in(keys[4], 71), 0),
        "range_bits": touch_ends(jax.random.randint(keys[2], (NBX, NBY, SLOTS, ST, WORDS), 0, 1073741824), jax.random.fold_in(keys[2], 1), 0, 1073741823).astype(jnp.int32),
        "old_stacks": centred(keys[3], (NBX, NBY, SLOTS, BANDS, 2, ST, ST), 1.0, 6.0, ((0, 4), (1, 8)), jnp.float32),
    }


EPSILON = 1e-06

def whiten(spectrum, band_count):
    segments, components, stations, freq_bins = spectrum.shape
    grouped = spectrum.astype(jnp.float32).reshape(segments, components, stations, band_count, freq_bins // band_count)
    band_power = lax.optimization_barrier(jnp.mean(grouped * grouped, axis=(0, 1, 4)))
    scaled = grouped * lax.rsqrt(band_power + EPSILON)[None, None, :, :, None]
    return scaled.reshape(spectrum.shape).astype(jnp.bfloat16)

def cross_bands(first_block, second_block, band_count):
    segments, components, stations, freq_bins = first_block.shape
    band_width = freq_bins // band_count
    first_wide = first_block.astype(jnp.float32)
    turned = jnp.stack([first_wide[:, 1], -first_wide[:, 0]], axis=1)
    stacked = jnp.stack([first_wide, turned], 0).reshape(2, segments, components, stations, band_count, band_width)
    partner_wide = second_block.astype(jnp.float32).reshape(segments, components, stations, band_count, band_width)
    product = jnp.einsum('oscinw,scjnw->noij', stacked, partner_wide, precision=lax.Precision.HIGHEST)
    return product * (1.0 / math.sqrt(segments * band_width))

def unpack_range(range_words, stations):
    word_count = range_words.shape[-1]
    column_ids = jnp.arange(stations, dtype=jnp.int32)
    onehot = (column_ids[:, None] // 30 == jnp.arange(word_count, dtype=jnp.int32)[None, :]).astype(jnp.int32)
    selected = lax.optimization_barrier(jnp.sum(range_words[..., :, None, :] * onehot, axis=-1))
    flags = jnp.bitwise_and(jnp.right_shift(selected, column_ids % 30), 1)
    return flags.astype(jnp.float32)

def reference(spectra, partner_codes, range_bits, old_stacks):
    row_count = spectra.shape[0]
    col_count = spectra.shape[1]
    block_count = row_count * col_count
    band_count = old_stacks.shape[3]
    stations = old_stacks.shape[-1]
    slot_count = partner_codes.shape[-1]
    flat_spectra = spectra.reshape((block_count,) + spectra.shape[2:])
    whitened = lax.map(lambda spectrum: whiten(spectrum, band_count), flat_spectra).reshape(spectra.shape)

    def per_block(item):
        block_index, code_row, range_words, old_block = item
        row_pos = block_index // col_count
        col_pos = block_index % col_count
        own_block = whitened[row_pos, col_pos]
        unit_zero = jnp.zeros((band_count, 2, stations, stations), jnp.float32)
        crosses = []
        for slot_index in range(slot_count):
            pair_code = code_row[slot_index]
            step_row = (pair_code == 1).astype(jnp.int32) + (pair_code == 4).astype(jnp.int32) - (pair_code == 2).astype(jnp.int32)
            step_col = (pair_code >= 2).astype(jnp.int32)
            target_row = jnp.clip(row_pos + step_row, 0, row_count - 1)
            target_col = jnp.clip(col_pos + step_col, 0, col_count - 1)
            partner_block = whitened[target_row, target_col]
            pair_cross = lax.cond(pair_code >= 0, lambda operands: cross_bands(operands[0], operands[1], band_count).astype(jnp.float32), lambda operands: unit_zero, (own_block, partner_block))
            crosses.append(pair_cross)
        cross_all = jnp.stack(crosses, 0)
        in_range = unpack_range(range_words, stations)
        return old_block + in_range[:, None, None] * cross_all
    flat_items = (jnp.arange(block_count, dtype=jnp.int32), partner_codes.reshape(block_count, slot_count), range_bits.reshape((block_count,) + range_bits.shape[2:]), old_stacks.reshape((block_count,) + old_stacks.shape[2:]))
    updated = lax.map(per_block, flat_items)
    return updated.reshape(old_stacks.shape)
```

```python
import math

import jax
import jax.numpy as jnp
from jax import lax
from jax.experimental import pallas as pl
from jax.experimental.pallas import tpu as pltpu
from jax.sharding import PartitionSpec as P

EPSILON = 1e-06
ROWS = 16
STEPS = 1024
LARGEST = 32767


def coded(value, top):
    base = LARGEST - STEPS * math.log2(top)
    size = jnp.log2(jnp.maximum(jnp.abs(value), 1e-30)) * STEPS + (base + 0.5)
    size = jnp.floor(jnp.clip(size, 0.0, float(LARGEST)))
    return jnp.where(value < 0.0, -size, size).astype(jnp.int32).astype(jnp.int16)


def decoded(code, top):
    base = LARGEST - STEPS * math.log2(top)
    wide = code.astype(jnp.int32).astype(jnp.float32)
    size = jnp.exp2((jnp.abs(wide) - base) * (1.0 / STEPS))
    return jnp.where(wide == 0.0, 0.0, jnp.where(wide < 0.0, -size, size))


def any_spec():
    return pl.BlockSpec(memory_space=pl.ANY)


def sent(value, mesh, target):
    rows, cols = mesh.shape["gx"], mesh.shape["gy"]
    pairs = []
    for x in range(rows):
        for y in range(cols):
            goal = target(x, y)
            if goal is not None and 0 <= goal[0] < rows and 0 <= goal[1] < cols:
                pairs.append((x * cols + y, goal[0] * cols + goal[1]))
    return lax.ppermute(value, ("gx", "gy"), pairs)


def whitened_bands(spectra, parity, first, count, bands):
    segs, parts, stations, bins = spectra.shape[2:]
    width = bins // bands
    share = 1.0 / (segs * parts * width)

    def kernel(parity_ref, source, *refs):
        outs, (loaded, scaled, in_sems, out_sems) = refs[:count], refs[count:]

        def load(k):
            band = lax.rem(first + k + parity_ref[0] * (bands // 2), bands)
            at = pl.multiple_of(band * width, 128)
            return pltpu.make_async_copy(
                source.at[0, 0, :, :, :, pl.ds(at, width)], loaded.at[k], in_sems.at[k])

        def store(k):
            return pltpu.make_async_copy(scaled.at[k], outs[k], out_sems.at[k])

        for k in range(count):
            load(k).start()
        for k in range(count):
            load(k).wait()

            def step(i, carry, k=k):
                rows = pl.ds(i * ROWS, ROWS)
                value = loaded[k, :, :, rows, :].astype(jnp.float32)
                total = jnp.sum(jnp.sum(value * value, axis=(0, 1)), axis=-1, keepdims=True)
                gain = lax.rsqrt(total * share + EPSILON)
                scaled[k, :, :, rows, :] = (value * gain[None, None]).astype(jnp.bfloat16)
                return carry

            lax.fori_loop(0, stations // ROWS, step, 0)
            store(k).start()
        for k in range(count):
            store(k).wait()

    block = (segs, parts, stations, width)
    return pl.pallas_call(
        kernel,
        grid_spec=pltpu.PrefetchScalarGridSpec(
            num_scalar_prefetch=1,
            grid=(),
            in_specs=[any_spec()],
            out_specs=[any_spec()] * count,
            scratch_shapes=[
                pltpu.VMEM((count,) + block, jnp.bfloat16),
                pltpu.VMEM((count,) + block, jnp.bfloat16),
                pltpu.SemaphoreType.DMA((count,)),
                pltpu.SemaphoreType.DMA((count,)),
            ],
        ),
        out_shape=[jax.ShapeDtypeStruct(block, jnp.bfloat16)] * count,
        name=f"whiten{first}",
    )(parity, spectra)


def pair_cross(first, second, factor):
    segs, parts, stations, width = first.shape
    total = None
    for s in range(segs):
        part = lax.dot_general(
            first[s].reshape(parts * stations, width),
            second[s].reshape(parts * stations, width),
            (((1,), (1,)), ((), ())),
            preferred_element_type=jnp.float32,
        )
        total = part if total is None else total + part
    real = total[:stations, :stations] + total[stations:, stations:]
    imag = total[stations:, :stations] - total[:stations, stations:]
    return real * factor, imag * factor


def packed_crosses(parity, places, edges, factor, top, name):
    operands = []
    wanted = []
    for even, odd in places:
        for array in (even, odd):
            if not any(array is known for known in operands):
                operands.append(array)
        wanted.append(tuple(
            next(n for n, known in enumerate(operands) if known is array) for array in (even, odd)))
    block = operands[0].shape
    stations = block[2]
    count = len(operands)

    def kernel(parity_ref, *refs):
        sources, outs = refs[:count], refs[count:count + len(edges)]
        held, sems = refs[count + len(edges):]
        odd = parity_ref[0] == 1

        def load(n, source):
            return pltpu.make_async_copy(sources[source], held.at[n], sems.at[n])

        for n, (even_at, odd_at) in enumerate(wanted):
            if even_at == odd_at:
                load(n, even_at).start()
            else:
                pl.when(odd)(lambda n=n, at=odd_at: load(n, at).start())
                pl.when(jnp.logical_not(odd))(lambda n=n, at=even_at: load(n, at).start())
        arrived = set()
        for out, members in zip(outs, edges):
            for k, pair in enumerate(members):
                for n in pair:
                    if n not in arrived:
                        load(n, wanted[n][0]).wait()
                        arrived.add(n)
                real, imag = pair_cross(held[pair[0]], held[pair[1]], factor)
                out[k, 0] = coded(real, top)
                out[k, 1] = coded(imag, top)

    return pl.pallas_call(
        kernel,
        grid_spec=pltpu.PrefetchScalarGridSpec(
            num_scalar_prefetch=1,
            grid=(),
            in_specs=[any_spec()] * count,
            out_specs=[pl.BlockSpec(memory_space=pltpu.VMEM)] * len(edges),
            scratch_shapes=[
                pltpu.VMEM((len(places),) + block, jnp.bfloat16),
                pltpu.SemaphoreType.DMA((len(places),)),
            ],
        ),
        out_shape=[
            jax.ShapeDtypeStruct((len(members), 2, stations, stations), jnp.int16)
            for members in edges
        ],
        name=name,
    )(parity, *operands)


def range_mask(words, stations):
    column = lax.broadcasted_iota(jnp.int32, (stations, stations), 1)
    chosen = jnp.zeros((stations, stations), jnp.int32)
    for w in range(words.shape[-1]):
        chosen = jnp.where(column // 30 == w, words[:, w:w + 1], chosen)
    return lax.bitwise_and(lax.shift_right_logical(chosen, column % 30), 1).astype(jnp.float32)


def own_slot(parity, whites, range_bits, old_stacks):
    slots, bands, parts, stations = old_stacks.shape[2:6]
    segs, _, _, width = whites[0].shape
    factor = 1.0 / math.sqrt(segs * width)

    def kernel(parity_ref, bits, old, *refs):
        sources, (out, held, sems) = refs[:bands], refs[bands:]
        step = pl.program_id(0)

        def load(n):
            return pltpu.make_async_copy(sources[n], held.at[n], sems.at[n])

        @pl.when(step == 0)
        def _():
            for n in range(bands):
                load(n).start()

        for n in range(bands):
            pl.when(step == n)(lambda n=n: load(n).wait())
        mask = range_mask(bits[0, 0, 0], stations)
        white = held[step]
        real, imag = pair_cross(white, white, factor)
        out[0, 0, 0, 0, 0] = old[0, 0, 0, 0, 0] + mask * real
        out[0, 0, 0, 0, 1] = old[0, 0, 0, 0, 1] + mask * imag

    def at(n, parity_ref):
        return (0, 0, 0, lax.rem(n + parity_ref[0] * (bands // 2), bands), 0, 0, 0)

    block = (1, 1, 1, 1, parts, stations, stations)
    return pl.pallas_call(
        kernel,
        grid_spec=pltpu.PrefetchScalarGridSpec(
            num_scalar_prefetch=1,
            grid=(bands,),
            in_specs=[
                pl.BlockSpec((1, 1, 1) + range_bits.shape[3:], lambda n, p: (0, 0, 0, 0, 0)),
                pl.BlockSpec(block, at),
            ] + [any_spec()] * bands,
            out_specs=pl.BlockSpec(block, at),
            scratch_shapes=[
                pltpu.VMEM((bands,) + whites[0].shape, jnp.bfloat16),
                pltpu.SemaphoreType.DMA((bands,)),
            ],
        ),
        out_shape=jax.ShapeDtypeStruct(old_stacks.shape, jnp.float32),
        name="own_slot",
    )(parity, range_bits, old_stacks, *whites)


def later_slots(parity, codes, range_bits, old_stacks, partial, pieces, top):
    slots, bands, parts, stations = old_stacks.shape[2:6]
    kinds = 1 + max(piece[3] for piece in pieces)
    operands = []
    placed = []
    for even, odd, index, code, band in pieces:
        numbers = []
        for array in (even, odd):
            if not any(array is known for known in operands):
                operands.append(array)
            numbers.append(next(n for n, known in enumerate(operands) if known is array))
        placed.append((numbers[0], numbers[1], index, code, band))
    count = len(operands)

    def kernel(parity_ref, code_ref, bits, old, partial_ref, *refs):
        sources, (out, held, sem) = refs[:count], refs[count:]
        odd = parity_ref[0] == 1

        def load(source, index, code, band):
            return pltpu.make_async_copy(
                sources[source].at[index], held.at[code - 1, band], sem.at[code - 1, band])

        @pl.when(pl.program_id(0) == 0)
        def _():
            for even_at, odd_at, index, code, band in placed:
                if even_at == odd_at:
                    load(even_at, index, code, band).start()
                else:
                    pl.when(odd)(lambda a=(odd_at, index, code, band): load(*a).start())
                    pl.when(jnp.logical_not(odd))(
                        lambda a=(even_at, index, code, band): load(*a).start())
            for even_at, odd_at, index, code, band in placed:
                load(even_at, index, code, band).wait()

        code = code_ref[pl.program_id(0) + 1]
        listed = (code > 0).astype(jnp.float32)
        kind = jnp.maximum(code, 1) - 1
        mask = range_mask(bits[0, 0, 0], stations) * listed

        def step(band, carry):
            at = lax.rem(band + parity_ref[0] * (bands // 2), bands)
            for part in range(parts):
                out[0, 0, 0, at, part] = (
                    old[0, 0, 0, at, part] + mask * decoded(held[kind, band, part], top))
            return carry

        lax.fori_loop(0, bands, step, 0)

    block = (1, 1, 1, bands, parts, stations, stations)
    at = lambda n, p, c: (0, 0, n + 1, 0, 0, 0, 0)
    return pl.pallas_call(
        kernel,
        grid_spec=pltpu.PrefetchScalarGridSpec(
            num_scalar_prefetch=2,
            grid=(slots - 1,),
            in_specs=[
                pl.BlockSpec((1, 1, 1) + range_bits.shape[3:], lambda n, p, c: (0, 0, n + 1, 0, 0)),
                pl.BlockSpec(block, at),
                any_spec(),
            ] + [any_spec()] * count,
            out_specs=pl.BlockSpec(block, at),
            scratch_shapes=[
                pltpu.VMEM((kinds - 1, bands, parts, stations, stations), jnp.int16),
                pltpu.SemaphoreType.DMA((kinds - 1, bands)),
            ],
        ),
        out_shape=jax.ShapeDtypeStruct(old_stacks.shape, jnp.float32),
        input_output_aliases={4: 0},
        name="later_slots",
    )(parity, codes, range_bits, old_stacks, partial, *operands)


def solution(mesh):
    partner = lambda x, y: (x, y ^ 1)
    home = lambda y: y if y % 2 == 0 else y - 2

    def body(spectra, partner_codes, range_bits, old_stacks):
        bands = old_stacks.shape[3]
        half, quarter = bands // 2, bands // 4
        segs, bins = spectra.shape[2], spectra.shape[5]
        width = bins // bands
        unit = math.sqrt(segs * width)
        factor = 1.0 / unit
        top = 2.2 * unit
        odd = lax.rem(lax.axis_index("gy"), 2).astype(jnp.int32)
        parity = odd.reshape(1)

        theirs = whitened_bands(spectra, parity, half, half, bands)
        swapped = {}
        for i in range(quarter):
            for l in (i, quarter + i):
                swapped[l] = sent(theirs[l], mesh, partner)
        mine = whitened_bands(spectra, parity, 0, half, bands)
        whites = list(mine) + list(theirs)
        further = {}
        near = {}
        for i in range(quarter):
            for l in (i, quarter + i):
                further[l] = sent(mine[l], mesh, lambda x, y: (x, y - 2 if y % 2 == 0 else y + 2))
                step = -1 if l < quarter else 1
                near[l] = sent(mine[l], mesh, lambda x, y: (x + step, y))
        for l in range(half, bands):
            step = -1 if l - half < quarter else 1
            near[l] = sent(whites[l], mesh, lambda x, y: (x + step, y))

        partial = own_slot(parity, whites, range_bits, old_stacks)

        below = [l for l in range(bands) if l % half < quarter]
        above = [l for l in range(bands) if l % half >= quarter]
        kept, owed = packed_crosses(
            parity,
            [(whites[l], whites[l]) for l in below + above]
            + [(near[l], near[l]) for l in below + above],
            [[(n, bands + n) for n in range(half)], [(bands + n, n) for n in range(half, bands)]],
            factor, top, "code1")
        returned = sent(owed, mesh, lambda x, y: (x - 1, y))
        pieces = [(kept, kept, n, 1, l) for n, l in enumerate(below)]
        pieces += [(returned, returned, n, 1, l) for n, l in enumerate(above)]

        for i in range(quarter):
            u, d = i, quarter + i
            step = {u: -1, d: 1}
            beside = {l: sent(swapped[l], mesh, lambda x, y: (x + step[l], y)) for l in (u, d)}
            beyond = {l: sent(further[l], mesh, lambda x, y: (x + step[l], y)) for l in (u, d)}
            places = []
            for l in (u, d):
                places += [(mine[l], further[l]), (swapped[l], swapped[l]), (further[l], mine[l])]
                places += [(near[l], beyond[l]), (beside[l], beside[l]), (beyond[l], near[l])]
            partner_kept, home_kept, partner_up, partner_down, home_up, home_down = packed_crosses(
                parity, places,
                [[(1, 2), (7, 8), (1, 5), (7, 11)],
                 [(0, 1), (6, 7), (0, 4), (6, 10)],
                 [(10, 8)], [(4, 2)], [(9, 7)], [(3, 1)]],
                factor, top, f"diagonals{i}")
            from_partner = sent(partner_kept, mesh, partner)
            from_home = sent(home_kept, mesh, lambda x, y: (x, y - 2) if y % 2 else None)
            partner_up = sent(partner_up, mesh, lambda x, y: (x - 1, y ^ 1))
            partner_down = sent(partner_down, mesh, lambda x, y: (x + 1, y ^ 1))
            home_up = sent(home_up, mesh, lambda x, y: (x - 1, home(y)))
            home_down = sent(home_down, mesh, lambda x, y: (x + 1, home(y)))
            pieces += [
                (home_kept, from_home, 0, 3, u), (home_kept, from_home, 1, 3, d),
                (home_kept, from_home, 2, 4, u), (home_kept, from_home, 3, 2, d),
                (home_up, home_up, 0, 4, d), (home_down, home_down, 0, 2, u),
                (from_partner, from_partner, 0, 3, half + u),
                (from_partner, from_partner, 1, 3, half + d),
                (from_partner, from_partner, 2, 4, half + u),
                (from_partner, from_partner, 3, 2, half + d),
                (partner_up, partner_up, 0, 4, half + d),
                (partner_down, partner_down, 0, 2, half + u),
            ]
        return later_slots(
            parity, partner_codes.reshape(-1), range_bits, old_stacks, partial, pieces, top)

    return jax.shard_map(
        body,
        mesh=mesh,
        in_specs=(
            P("gx", "gy", None, None, None, None),
            P("gx", "gy", None),
            P("gx", "gy", None, None, None),
            P("gx", "gy", None, None, None, None, None),
        ),
        out_specs=P("gx", "gy", None, None, None, None, None),
        check_vma=False,
    )
```
